256 devices in a mesh: sector: 16 (over y, x), term: 16 (over z, core).
Axes of the slice: x: 4, y: 4, z: 8, core: 2. Of those that a mesh axis runs over, the one named last changes fastest.
Arguments:
- wavefunction: float32 [16, 256, 256], P('sector'), may hold values from -6 to 6
- left_env: float32 [3072, 256, 256], P(('sector', 'term')), may hold values from -0.02734375 to 0.02734375
- right_env: float32 [3072, 256, 256], P(('sector', 'term')), may hold values from -0.375 to 0.375
- in_sector: int32 [3072], P(('sector', 'term')), may hold values from 0 to 15
- out_sector: int32 [3072], P(('sector', 'term')), may hold values from 0 to 15
- precond: float32 [16, 256, 256], P('sector'), may hold values from 2 to 4
- shifts: float32 [2], replicated, may hold values from 0.2 to 1
Outputs:
- corrected: float32 [16, 256, 256], P('sector')
- residual_norms: float32 [2], replicated
The draws below stay inside these ranges and needn't reach their ends.
All inputs are finite; a program needn't handle non-finite values.
Results may differ from the reference program's by a relative error of at most 0.0001.
Values sent between devices are 32-bit elements; how exact they have to be, the bound alone decides.
No kernel may reach another device: no remote copies, remote signals or barrier semaphores. Data moves between devices by JAX's collectives and lax.ppermute only.
A program may use at most 64 MiB of HBM per device.

```python
import math
import jax
import jax.numpy as jnp
import numpy as np
from jax import lax

B = 256
SEC_DEV = 1
TASK_DEV = 12
ITERS = 2
SECTORS = 16
TASKS = 3072
N_TERM = 16


def touch_ends(drawn, own_key, smallest, top_value):
    spot = [jax.random.randint(jax.random.fold_in(own_key, axis), (), 0, length) for axis, length in enumerate(drawn.shape)]
    main_axis = drawn.shape.index(max(drawn.shape))
    next_to = spot[:main_axis] + [(spot[main_axis] + 1) % drawn.shape[main_axis]] + spot[main_axis + 1:]
    return drawn.at[tuple(spot)].set(smallest).at[tuple(next_to)].set(top_value)


def block_scale(rng, dims, pieces, low, high):
    def one(position, shards_of):
        heights = jax.random.uniform(jax.random.fold_in(jax.random.fold_in(rng, 6), position), (shards_of,), jnp.float32, low / len(pieces), high / len(pieces))
        return jnp.repeat(jnp.exp(heights), dims[position] // shards_of).reshape((-1,) + (1,) * (len(dims) - position - 1))

    factor_of = one(*pieces[0])
    for cut in pieces[1:]:
        factor_of = factor_of * one(*cut)
    return factor_of


def cumulative_ranks(amount, slope):
    loads = [(1 << 20) // math.isqrt(rank ** slope) + 1 for rank in range(1, amount + 1)]
    scale = 1 + sum(loads) // (1 << 30)
    return np.cumsum(np.array([max(1, weight // scale) for weight in loads]))


def ranked(rng, dims, count, lean):
    listing = cumulative_ranks(count, lean)
    lot = jax.random.randint(jax.random.fold_in(rng, 1), dims, 0, int(listing[count - 1]))
    rank = jnp.searchsorted(jnp.asarray(listing, jnp.int32), lot, side="right")
    return jax.random.permutation(jax.random.fold_in(rng, 2), count)[rank].astype(jnp.int32)


def scatter_about(key, dims, spread, bound, pieces=(), held_as=jnp.bfloat16):
    entries = spread * jax.random.normal(key, dims, jnp.float32)
    if pieces:
        entries = entries * block_scale(key, dims, pieces, -0.22, 0.18)
    return jnp.clip(entries, -bound, bound).astype(held_as)


def setup_inputs(seed: int = 0) -> dict:
    keys = jax.random.split(jax.random.key(seed), 8)
    wavefunction = scatter_about(keys[0], (SECTORS, B, B), 1.0, 6.0, ((0, 16),), jnp.float32)
    left_env = scatter_about(keys[1], (TASKS, B, B), (B * TASK_DEV * N_TERM // SEC_DEV) ** -0.5, 0.02734375, ((0, 256),), jnp.float32)
    right_env = scatter_about(keys[2], (TASKS, B, B), B ** -0.5, 0.375, ((0, 256),), jnp.float32)
    in_sector = touch_ends(ranked(keys[3], (TASKS,), SECTORS, 1), jax.random.fold_in(keys[3], 3), 0, SECTORS - 1).astype(jnp.int32)
    out_sector = touch_ends(jax.random.randint(keys[4], (TASKS,), 0, SECTORS), jax.random.fold_in(keys[4], 1), 0, SECTORS - 1).astype(jnp.int32)
    precond = jnp.clip(2.0 + 2.0 * jax.random.uniform(keys[5], (SECTORS, B, B), jnp.float32) ** block_scale(keys[5], (SECTORS, B, B), ((0, 16),), -0.2, 0.2), 2.0, 4.0)
    shifts = jnp.clip(jax.random.uniform(keys[6], (ITERS,), jnp.float32, 0.2, 1.0), 0.2, 1.0)
    return {"wavefunction": wavefunction, "left_env": left_env, "right_env": right_env, "in_sector": in_sector, "out_sector": out_sector, "precond": precond, "shifts": shifts}


def apply_tasks(full, left_env, right_env, in_sector, out_sector):

    def one_task(total, item):
        left, right, source, target = item
        block = lax.dynamic_index_in_dim(full, source, 0, keepdims=False)
        middle = jnp.dot(left, block, precision=lax.Precision.HIGHEST, preferred_element_type=jnp.float32)
        result = jnp.dot(middle, right, precision=lax.Precision.HIGHEST, preferred_element_type=jnp.float32)
        current = lax.dynamic_index_in_dim(total, target, 0, keepdims=False)
        total = lax.dynamic_update_index_in_dim(total, current + result, target, 0)
        return (total, None)
    start = jnp.zeros(full.shape, jnp.float32)
    total, _ = lax.scan(one_task, start, (left_env, right_env, in_sector, out_sector))
    return total

def reference(wavefunction, left_env, right_env, in_sector, out_sector, precond, shifts):
    psi = wavefunction
    norms = []
    for step in range(ITERS):
        sigma = apply_tasks(psi, left_env, right_env, in_sector, out_sector)
        residual = sigma - shifts[step] * psi
        norms.append(jnp.sqrt(jnp.sum(residual * residual)))
        updated = psi - residual / (precond - shifts[step])
        psi = updated / jnp.sqrt(jnp.mean(updated * updated) + 1e-06)
    return (psi, jnp.stack(norms))
```

```python
import jax
import jax.numpy as jnp
from jax import lax
from jax.experimental import pallas as pl
from jax.experimental.pallas import tpu as pltpu
from jax.sharding import Mesh
from jax.sharding import PartitionSpec as P

ITERS = 2
SECTOR = ("sector_0", "sector_1")
SECTOR_TERM = ("sector_0", "sector_1", "term")
EVERY = ("term", "sector_0", "sector_1")


def split(value):
    high = value.astype(jnp.bfloat16)
    return high, (value - high.astype(jnp.float32)).astype(jnp.bfloat16)


def product(left, right):
    left_high, left_low = split(left)
    right_high, right_low = split(right)

    def part(a, b):
        return jnp.dot(a, b, preferred_element_type=jnp.float32)

    return part(left_high, right_high) + (part(left_low, right_high) + part(left_high, right_low))


def task_body(source, target, psi, left, right, total):
    step = pl.program_id(0)

    @pl.when(step == 0)
    def _():
        total[...] = jnp.zeros_like(total)

    total[target[step]] += product(product(left[0], psi[0]), right[0])


def apply_tasks(full, left_env, right_env, in_sector, out_sector):
    tasks, rows, cols = left_env.shape
    block = (1, rows, cols)
    return pl.pallas_call(
        task_body,
        grid_spec=pltpu.PrefetchScalarGridSpec(
            num_scalar_prefetch=2,
            grid=(tasks,),
            in_specs=[
                pl.BlockSpec(block, lambda t, source, target: (source[t], 0, 0)),
                pl.BlockSpec(block, lambda t, source, target: (t, 0, 0)),
                pl.BlockSpec(block, lambda t, source, target: (t, 0, 0)),
            ],
            out_specs=pl.BlockSpec(full.shape, lambda t, source, target: (0, 0, 0)),
        ),
        out_shape=jax.ShapeDtypeStruct(full.shape, jnp.float32),
        compiler_params=pltpu.CompilerParams(
            dimension_semantics=("arbitrary",), vmem_limit_bytes=24 << 20
        ),
        cost_estimate=pl.CostEstimate(
            flops=12 * tasks * rows * rows * cols,
            bytes_accessed=4 * (3 * tasks * rows * cols + full.size),
            transcendentals=0,
        ),
        name="tasks",
    )(in_sector, out_sector, full, left_env, right_env)


def per_device(wavefunction, left_env, right_env, in_sector, out_sector, precond, shifts):
    full = lax.all_gather(wavefunction, SECTOR, axis=0, tiled=True)
    norms = []
    psi = wavefunction
    count = lax.axis_size(SECTOR) * psi.size
    for step in range(ITERS):
        partial_value = apply_tasks(full, left_env, right_env, in_sector, out_sector)
        owned = lax.psum_scatter(partial_value, SECTOR, scatter_dimension=0, tiled=True)
        sigma = lax.all_gather(owned, "term").sum(axis=0)
        shift = shifts[step]
        residual = sigma - shift * psi
        updated = psi - residual / (precond - shift)
        sums = lax.psum(jnp.stack([jnp.sum(residual * residual), jnp.sum(updated * updated)]), SECTOR)
        norms.append(jnp.sqrt(sums[0]))
        psi = updated / jnp.sqrt(sums[1] / count + 1e-06)
        if step + 1 < ITERS:
            full = lax.all_gather(psi, SECTOR, axis=0, tiled=True)
    return (psi, jnp.stack(norms))


def solution(mesh):
    torus = Mesh(mesh.devices.reshape(4, 4, mesh.shape["term"]), ("sector_0", "sector_1", "term"))
    placed = (
        P(SECTOR, None, None),
        P(SECTOR_TERM, None, None),
        P(SECTOR_TERM, None, None),
        P(SECTOR_TERM),
        P(SECTOR_TERM),
        P(SECTOR, None, None),
        P(),
    )
    return jax.shard_map(
        per_device,
        mesh=torus,
        in_specs=placed,
        out_specs=(P(SECTOR, None, None), P()),
        check_vma=False,
    )
```

```python
import functools

import jax
import jax.numpy as jnp
from jax import lax
from jax.experimental import pallas as pl
from jax.experimental.pallas import tpu as pltpu
from jax.sharding import Mesh
from jax.sharding import PartitionSpec as P

ITERS = 2
AXES = ("y", "x", "z", "c")
SECTOR = ("y", "x")
SECTOR_TERM = ("y", "x", "z", "c")
NY, NX, NZ, NC = 4, 4, 8, 2
EPS = 1e-06
SUMS = 8


VMEM = pl.BlockSpec(memory_space=pltpu.VMEM)
SMEM = pl.BlockSpec(memory_space=pltpu.SMEM)
HBM = pl.BlockSpec(memory_space=pltpu.HBM)


def f32(*shape):
    return jax.ShapeDtypeStruct(shape, jnp.float32)


def local(body, name, outs, in_specs, args, scratch=(), flops=0, limit=16 << 20):
    moved = sum(4 * a.size for a in args) + sum(4 * o.size for o in outs)
    return pl.pallas_call(
        body,
        out_shape=tuple(outs),
        in_specs=in_specs,
        out_specs=tuple(VMEM for _ in outs),
        scratch_shapes=list(scratch),
        compiler_params=pltpu.CompilerParams(vmem_limit_bytes=limit),
        cost_estimate=pl.CostEstimate(
            flops=max(flops, moved), bytes_accessed=moved, transcendentals=0
        ),
        name=name,
    )(*args)


def shift_by(value, axis, by):
    size = {"y": NY, "x": NX, "z": NZ, "c": NC}[axis]
    return lax.ppermute(value, axis, [(i, (i + by) % size) for i in range(size)])


def split(value):
    high = value.astype(jnp.bfloat16)
    return high, (value - high.astype(jnp.float32)).astype(jnp.bfloat16)


def product(left, right):
    left_high, left_low = split(left)
    right_high, right_low = split(right)

    def part(a, b):
        return jnp.dot(a, b, preferred_element_type=jnp.float32)

    return part(left_high, right_high) + (part(left_low, right_high) + part(left_high, right_low))


def tasks_body(tasks, half, coords, source, target, left_hbm, right_hbm, *refs):
    pieces, (own, peer, square), (psi, left, right, left_sem, right_sem) = (
        refs[:16],
        refs[16:19],
        refs[19:],
    )
    core = coords[1]

    def copies(t):
        return (
            pltpu.make_async_copy(left_hbm.at[t], left.at[t], left_sem.at[t]),
            pltpu.make_async_copy(right_hbm.at[t], right.at[t], right_sem.at[t]),
        )

    @pl.loop(0, tasks)
    def _(t):
        for copy in copies(t):
            copy.start()

    own[...] = jnp.zeros_like(own)
    peer[...] = jnp.zeros_like(peer)
    quarter = half // 2
    squares = jnp.zeros((quarter, psi.shape[-1]), jnp.float32)
    for side in range(2):
        base = jnp.where(side == 0, core, 1 - core) * half
        for k in range(4):
            for part in range(2):
                rows = pl.ds(pl.multiple_of(base + part * quarter, quarter), quarter)
                piece = pieces[side * 8 + part * 4 + k]
                for j in range(4):
                    value = piece[j]
                    slot = k * 4 + j if part == 0 else j * 4 + k
                    psi[slot, rows, :] = value
                    squares += value * value
    square[...] = jnp.full(square.shape, jnp.sum(squares), jnp.float32)

    mine = pl.ds(pl.multiple_of(core * half, half), half)
    other = pl.ds(pl.multiple_of((1 - core) * half, half), half)

    @pl.loop(0, tasks)
    def _(t):
        for copy in copies(t):
            copy.wait()
        rows = jnp.concatenate([left[t, mine, :], left[t, other, :]], axis=0)
        result = product(product(rows, psi[source[t]]), right[t])
        goal = target[t]
        own[goal] += result[:half]
        peer[goal] += result[half:]


def apply_tasks(pieces, left_env, right_env, in_slot, out_slot, coords):
    tasks, rows, cols = left_env.shape
    half = rows // 2
    return local(
        functools.partial(tasks_body, tasks, half),
        "tasks",
        [f32(16, half, cols), f32(16, half, cols), f32(8, 128)],
        [SMEM, SMEM, SMEM, HBM, HBM] + [VMEM] * 16,
        [coords, in_slot, out_slot, left_env, right_env, *pieces],
        scratch=[
            pltpu.VMEM((16, rows, cols), jnp.float32),
            pltpu.VMEM(left_env.shape, jnp.float32),
            pltpu.VMEM(right_env.shape, jnp.float32),
            pltpu.SemaphoreType.DMA((tasks,)),
            pltpu.SemaphoreType.DMA((tasks,)),
        ],
        flops=12 * tasks * rows * rows * cols,
        limit=32 << 20,
    )


def join_cores_body(own, got, *outs):
    quarter = outs[0].shape[1]
    for k in range(4):
        for j in range(4):
            a = k * 4 + j
            outs[k][j] = own[a, :quarter] + got[a, :quarter]
            b = j * 4 + k
            outs[4 + k][j] = own[b, quarter:] + got[b, quarter:]


def sum_first_body(*refs):
    a, b, outs = refs[:4], refs[4:8], refs[8:]
    for j in range(4):
        outs[j][...] = (a[0][j] + a[1][j]) + (a[2][j] + a[3][j])
        outs[4 + j][...] = (b[0][j] + b[1][j]) + (b[2][j] + b[3][j])


def sum_second_body(coords, *refs):
    a, b, outs, half = refs[:4], refs[4:8], refs[8:16], refs[16]
    quarter = a[0].shape[0]
    half[:quarter] = (a[0][...] + a[1][...]) + (a[2][...] + a[3][...])
    half[quarter:] = (b[0][...] + b[1][...]) + (b[2][...] + b[3][...])
    rows = outs[0].shape[0]
    for k in range(NZ):
        to = lax.rem(coords[0] + k, NZ)
        outs[k][...] = half[pl.ds(pl.multiple_of(to * rows, rows), rows), :]


def reduce_to_piece(own, peer, coords):
    _, half, cols = own.shape
    quarter, rows = half // 2, half // NZ
    got = shift_by(peer, "c", 1)
    first = local(
        join_cores_body, "join_cores", [f32(4, quarter, cols)] * 8, [VMEM] * 2, [own, got]
    )
    a = [first[0]] + [shift_by(first[k], "y", k) for k in (1, 2, 3)]
    b = [first[4]] + [shift_by(first[4 + k], "x", k) for k in (1, 2, 3)]
    second = local(sum_first_body, "sum_first", [f32(quarter, cols)] * 8, [VMEM] * 8, a + b)
    a = [second[0]] + [shift_by(second[k], "x", k) for k in (1, 2, 3)]
    b = [second[4]] + [shift_by(second[4 + k], "y", k) for k in (1, 2, 3)]
    third = local(
        sum_second_body,
        "sum_second",
        [f32(rows, cols)] * NZ,
        [SMEM] + [VMEM] * 8,
        [coords] + a + b,
        scratch=[pltpu.VMEM((half, cols), jnp.float32)],
    )
    return [third[0]] + [shift_by(third[k], "z", k) for k in range(1, NZ)]


def total(value):
    return jnp.sum(jnp.sum(value, axis=1, keepdims=True), axis=0, keepdims=True)


def own_rows(coords, half, rows):
    return pl.ds(pl.multiple_of(coords[1] * half + coords[0] * rows, rows), rows)


def first_update_body(half, coords, shifts, psi, precond, *refs):
    parts, (updated_ref, sums_ref) = refs[:NZ], refs[NZ:]
    rows = parts[0].shape[0]
    here = own_rows(coords, half, rows)
    sigma = functools.reduce(lambda p, q: p + q, [p[...] for p in parts])
    shift = shifts[0]
    current = psi[0, here, :]
    residual = sigma - shift * current
    updated_ref[...] = current - residual / (precond[0, here, :] - shift)
    sums_ref[...] = jnp.broadcast_to(total(residual * residual), sums_ref.shape)


def second_update_body(half, count, coords, shifts, square, before, sums, precond, *refs):
    parts, (out,) = refs[:NZ], refs[NZ:]
    rows = parts[0].shape[0]
    here = own_rows(coords, half, rows)
    norm = jnp.sqrt(square[...] / count + EPS)[:1, :1]
    sigma = functools.reduce(lambda p, q: p + q, [p[...] for p in parts]) / norm
    shift = shifts[1]
    current = before[...] / norm
    residual = sigma - shift * current
    updated = current - residual / (precond[0, here, :] - shift)
    out[:rows] = updated
    line = lax.broadcasted_iota(jnp.int32, sums.shape, 0)
    out[rows:] = jnp.where(
        line == 0,
        sums[...],
        jnp.where(line == 1, total(residual * residual), total(updated * updated)),
    )


def place_body(coords, *refs):
    pieces, (a, b), half = refs[:NZ], refs[NZ : NZ + 2], refs[NZ + 2]
    rows = pieces[0].shape[0]
    for k in range(NZ):
        origin = lax.rem(coords[0] + NZ - k, NZ)
        half[pl.ds(pl.multiple_of(origin * rows, rows), rows), :] = pieces[k][...]
    quarter = a.shape[0]
    a[...] = half[:quarter]
    b[...] = half[quarter:]


def place_last_body(coords, *refs):
    pieces, out, sums = refs[:NZ], refs[NZ], refs[NZ + 1]
    rows = pieces[0].shape[0] - SUMS
    for k in range(NZ):
        origin = lax.rem(coords[0] + NZ - k, NZ)
        out[pl.ds(pl.multiple_of(origin * rows, rows), rows), :] = pieces[k][:rows]
        sums[origin] = pieces[k][rows:]
    out[NZ * rows :] = functools.reduce(lambda p, q: p + q, [sums[k] for k in range(NZ)])


def join_sums_body(which, size, coords, *refs):
    parts, out, sums = refs[:size], refs[size], refs[size + 1]
    for k in range(size):
        sums[lax.rem(coords[which] + size - k, size)] = parts[k][...]
    out[...] = functools.reduce(lambda p, q: p + q, [sums[k] for k in range(size)])


def finish_body(count, coords, mine, other, *refs):
    parts, (out, norms), sums = refs[:NY], refs[NY : NY + 2], refs[NY + 2]
    for k in range(NY):
        sums[lax.rem(coords[2] + NY - k, NY)] = parts[k][...]
    whole = functools.reduce(lambda p, q: p + q, [sums[k] for k in range(NY)])
    norms[...] = jnp.sqrt(whole)
    norm = jnp.sqrt(whole / count + EPS)[2:3, :1]
    half = out.shape[1] // 2
    out[0, pl.ds(pl.multiple_of(coords[1] * half, half), half), :] = mine[:half] / norm
    out[0, pl.ds(pl.multiple_of((1 - coords[1]) * half, half), half), :] = other[:half] / norm


def spread(a, b):
    across = jnp.stack([a] + [shift_by(a, "x", k) for k in (1, 2, 3)])
    along = jnp.stack([b] + [shift_by(b, "y", k) for k in (1, 2, 3)])
    pieces = [across] + [shift_by(across, "y", k) for k in (1, 2, 3)]
    pieces += [along] + [shift_by(along, "x", k) for k in (1, 2, 3)]
    return pieces + [shift_by(piece, "c", 1) for piece in pieces]


def per_device(wavefunction, left_env, right_env, in_sector, out_sector, precond, shifts):
    y, x, z, c = (lax.axis_index(name) for name in AXES)
    coords = jnp.stack([z, c, y, x]).astype(jnp.int32)
    in_slot = ((y - in_sector // NX) % NY) * NX + (x - in_sector % NX) % NX
    out_slot = ((out_sector // NX - y) % NY) * NX + (out_sector % NX - x) % NX
    _, size, cols = wavefunction.shape
    half, rows = size // 2, size // 2 // NZ
    count = NY * NX * size * cols

    def tasks(pieces):
        return apply_tasks(pieces, left_env, right_env, in_slot, out_slot, coords)

    mine = lax.dynamic_slice_in_dim(wavefunction[0], c * half, half, 0)
    own, peer, _ = tasks(spread(mine[: half // 2], mine[half // 2 :]))
    parts = reduce_to_piece(own, peer, coords)
    updated, sums = local(
        functools.partial(first_update_body, half),
        "first_update",
        [f32(rows, cols), f32(SUMS, cols)],
        [SMEM, SMEM] + [VMEM] * (2 + NZ),
        [coords, shifts, wavefunction, precond, *parts],
    )
    pieces = [updated] + [shift_by(updated, "z", k) for k in range(1, NZ)]
    a, b = local(
        place_body,
        "place",
        [f32(half // 2, cols)] * 2,
        [SMEM] + [VMEM] * NZ,
        [coords, *pieces],
        scratch=[pltpu.VMEM((half, cols), jnp.float32)],
    )
    own, peer, square = tasks(spread(a, b))
    parts = reduce_to_piece(own, peer, coords)
    (piece,) = local(
        functools.partial(second_update_body, half, count),
        "second_update",
        [f32(rows + SUMS, cols)],
        [SMEM, SMEM] + [VMEM] * (4 + NZ),
        [coords, shifts, square, updated, sums, precond, *parts],
    )
    pieces = [piece] + [shift_by(piece, "z", k) for k in range(1, NZ)]
    (mine,) = local(
        place_last_body,
        "place_last",
        [f32(half + SUMS, cols)],
        [SMEM] + [VMEM] * NZ,
        [coords, *pieces],
        scratch=[pltpu.VMEM((NZ, SUMS, cols), jnp.float32)],
    )
    other = shift_by(mine, "c", 1)
    sums = mine[half:] + other[half:]
    (sums,) = local(
        functools.partial(join_sums_body, 3, NX),
        "join_sums",
        [f32(SUMS, cols)],
        [SMEM] + [VMEM] * NX,
        [coords, sums] + [shift_by(sums, "x", k) for k in (1, 2, 3)],
        scratch=[pltpu.VMEM((NX, SUMS, cols), jnp.float32)],
    )
    psi, norms = local(
        functools.partial(finish_body, count),
        "finish",
        [f32(1, size, cols), f32(SUMS, cols)],
        [SMEM] + [VMEM] * (2 + NY),
        [coords, mine, other, sums] + [shift_by(sums, "y", k) for k in (1, 2, 3)],
        scratch=[pltpu.VMEM((NY, SUMS, cols), jnp.float32)],
    )
    return psi, norms[:ITERS, 0]


def solution(mesh):
    torus = Mesh(mesh.devices.reshape(NY, NX, NZ, NC), AXES)
    placed = (
        P(SECTOR, None, None),
        P(SECTOR_TERM, None, None),
        P(SECTOR_TERM, None, None),
        P(SECTOR_TERM),
        P(SECTOR_TERM),
        P(SECTOR, None, None),
        P(),
    )
    return jax.shard_map(
        per_device,
        mesh=torus,
        in_specs=placed,
        out_specs=(P(SECTOR, None, None), P()),
        check_vma=False,
    )
```

```python
import functools

import jax
import jax.numpy as jnp
from jax import lax
from jax.experimental import pallas as pl
from jax.experimental.pallas import tpu as pltpu
from jax.sharding import Mesh
from jax.sharding import PartitionSpec as P

ITERS = 2
AXES = ("y", "x", "z", "c")
SECTOR = ("y", "x")
SECTOR_TERM = ("y", "x", "z", "c")
NY, NX, NZ, NC = 4, 4, 8, 2
EPS = 1e-06
SUMS = 8


VMEM = pl.BlockSpec(memory_space=pltpu.VMEM)
SMEM = pl.BlockSpec(memory_space=pltpu.SMEM)
HBM = pl.BlockSpec(memory_space=pltpu.HBM)


def f32(*shape):
    return jax.ShapeDtypeStruct(shape, jnp.float32)


def local(body, name, outs, in_specs, args, scratch=(), flops=0, limit=16 << 20):
    moved = sum(4 * a.size for a in args) + sum(4 * o.size for o in outs)
    return pl.pallas_call(
        body,
        out_shape=tuple(outs),
        in_specs=in_specs,
        out_specs=tuple(VMEM for _ in outs),
        scratch_shapes=list(scratch),
        compiler_params=pltpu.CompilerParams(vmem_limit_bytes=limit),
        cost_estimate=pl.CostEstimate(
            flops=max(flops, moved), bytes_accessed=moved, transcendentals=0
        ),
        name=name,
    )(*args)


def shift_by(value, axis, by):
    size = {"y": NY, "x": NX, "z": NZ, "c": NC}[axis]
    return lax.ppermute(value, axis, [(i, (i + by) % size) for i in range(size)])


def split(value):
    high = value.astype(jnp.bfloat16)
    return high, (value - high.astype(jnp.float32)).astype(jnp.bfloat16)


def product(left, right):
    def part(a, b):
        return jnp.dot(a, b, preferred_element_type=jnp.float32)

    return part(left[0], right[0]) + (part(left[1], right[0]) + part(left[0], right[1]))


def split_body(coords, left, right, left_high, left_low, right_high, right_low):
    half = left.shape[1] // 2
    for side in range(2):
        base = jnp.where(side == 0, coords[1], 1 - coords[1]) * half
        rows = left[0, pl.ds(pl.multiple_of(base, half), half), :]
        there = slice(side * half, (side + 1) * half)
        left_high[0, there], left_low[0, there] = split(rows)
    right_high[0], right_low[0] = split(right[0])


def split_env(left_env, right_env, coords):
    block = pl.BlockSpec((1, *left_env.shape[1:]), lambda t: (t, 0, 0))
    return pl.pallas_call(
        split_body,
        grid=(left_env.shape[0],),
        out_shape=(jax.ShapeDtypeStruct(left_env.shape, jnp.bfloat16),) * 4,
        in_specs=[SMEM, block, block],
        out_specs=(block,) * 4,
        compiler_params=pltpu.CompilerParams(
            dimension_semantics=("arbitrary",), vmem_limit_bytes=8 << 20
        ),
        cost_estimate=pl.CostEstimate(
            flops=100 * left_env.size, bytes_accessed=16 * left_env.size, transcendentals=0
        ),
        name="split_env",
    )(coords, left_env, right_env)


def tasks_body(tasks, half, coords, source, target, *refs):
    envs, pieces, (own, peer, square), (psi_high, psi_low) = (
        refs[:4],
        refs[4:20],
        refs[20:23],
        refs[23:],
    )
    left_high, left_low, right_high, right_low = envs
    own[...] = jnp.zeros_like(own)
    peer[...] = jnp.zeros_like(peer)
    quarter = half // 2
    squares = jnp.zeros((quarter, psi_high.shape[-1]), jnp.float32)
    for side in range(2):
        base = jnp.where(side == 0, coords[1], 1 - coords[1]) * half
        for k in range(4):
            for part in range(2):
                rows = pl.ds(pl.multiple_of(base + part * quarter, quarter), quarter)
                piece = pieces[side * 8 + part * 4 + k]
                for j in range(4):
                    value = piece[j]
                    up, over = (k, j) if part == 0 else (j, k)
                    slot = lax.rem(coords[2] + NY - up, NY) * NX + lax.rem(coords[3] + NX - over, NX)
                    psi_high[slot, rows, :], psi_low[slot, rows, :] = split(value)
                    squares += value * value
    square[...] = jnp.full(square.shape, jnp.sum(squares), jnp.float32)

    @pl.loop(0, tasks, unroll=2)
    def _(t):
        slot, goal = source[t], target[t]
        middle = product((left_high[t], left_low[t]), (psi_high[slot], psi_low[slot]))
        result = product(split(middle), (right_high[t], right_low[t]))
        own[goal] += result[:half]
        peer[goal] += result[half:]


def apply_tasks(pieces, envs, in_sector, out_sector, coords):
    tasks, rows, cols = envs[0].shape
    half = rows // 2
    return local(
        functools.partial(tasks_body, tasks, half),
        "tasks",
        [f32(16, half, cols), f32(16, half, cols), f32(8, 128)],
        [SMEM, SMEM, SMEM] + [VMEM] * 20,
        [coords, in_sector, out_sector, *envs, *pieces],
        scratch=[pltpu.VMEM((16, rows, cols), jnp.bfloat16)] * 2,
        flops=12 * tasks * rows * rows * cols,
        limit=28 << 20,
    )


def add(values):
    return functools.reduce(lambda p, q: p + q, list(values))


def exchange(value, axis):
    return lax.all_to_all(value, axis, split_axis=0, concat_axis=0, tiled=True)


def join_cores_body(coords, own, got, *outs):
    quarter = outs[0].shape[1]
    for k in range(4):
        up = lax.rem(coords[2] + k, NY)
        over = lax.rem(coords[3] + k, NX)
        for j in range(4):
            slot = up * NX + j
            outs[k][j] = own[slot, :quarter] + got[slot, :quarter]
            slot = j * NX + over
            outs[4 + k][j] = own[slot, quarter:] + got[slot, quarter:]


def sum_first_body(*refs):
    a, b, (a_out, b_out) = refs[:4], refs[4:8], refs[8:]
    a_out[...] = add(ref[...] for ref in a)
    b_out[...] = add(ref[...] for ref in b)


def sum_second_body(a, b, out):
    quarter = a.shape[1]
    per = NZ // 2
    rows = quarter // per
    for where, ref in ((0, a), (per, b)):
        value = add(ref[k] for k in range(4))
        for k in range(per):
            out[where + k] = value[k * rows : (k + 1) * rows]


def reduce_to_piece(own, peer, coords):
    _, half, cols = own.shape
    quarter, rows = half // 2, half // NZ
    got = shift_by(peer, "c", 1)
    first = local(
        join_cores_body,
        "join_cores",
        [f32(4, quarter, cols)] * 8,
        [SMEM] + [VMEM] * 2,
        [coords, own, got],
    )
    a = [first[0]] + [shift_by(first[k], "y", k) for k in (1, 2, 3)]
    b = [first[4]] + [shift_by(first[4 + k], "x", k) for k in (1, 2, 3)]
    a, b = local(sum_first_body, "sum_first", [f32(4, quarter, cols)] * 2, [VMEM] * 8, a + b)
    a, b = exchange(a, "x"), exchange(b, "y")
    (rows_of,) = local(sum_second_body, "sum_second", [f32(NZ, rows, cols)], [VMEM] * 2, [a, b])
    return exchange(rows_of, "z")


def total(value):
    return jnp.sum(jnp.sum(value, axis=1, keepdims=True), axis=0, keepdims=True)


def own_rows(coords, half, rows):
    return pl.ds(pl.multiple_of(coords[1] * half + coords[0] * rows, rows), rows)


def first_update_body(half, coords, shifts, psi, precond, parts, updated_ref, sums_ref):
    here = own_rows(coords, half, parts.shape[1])
    sigma = add(parts[k] for k in range(NZ))
    shift = shifts[0]
    current = psi[0, here, :]
    residual = sigma - shift * current
    updated_ref[...] = current - residual / (precond[0, here, :] - shift)
    sums_ref[...] = jnp.broadcast_to(total(residual * residual), sums_ref.shape)


def second_update_body(half, count, coords, shifts, square, before, sums, precond, parts, out):
    rows = parts.shape[1]
    here = own_rows(coords, half, rows)
    norm = jnp.sqrt(square[...] / count + EPS)[:1, :1]
    sigma = add(parts[k] for k in range(NZ)) / norm
    shift = shifts[1]
    current = before[...] / norm
    residual = sigma - shift * current
    updated = current - residual / (precond[0, here, :] - shift)
    out[:rows] = updated
    line = lax.broadcasted_iota(jnp.int32, sums.shape, 0)
    out[rows:] = jnp.where(
        line == 0,
        sums[...],
        jnp.where(line == 1, total(residual * residual), total(updated * updated)),
    )


def place_last_body(pieces, out):
    rows = pieces.shape[1] - SUMS
    for k in range(NZ):
        out[k * rows : (k + 1) * rows] = pieces[k, :rows]
    out[NZ * rows :] = add(pieces[k, rows:] for k in range(NZ))


def join_sums_body(mine, other, out):
    out[...] = mine[mine.shape[0] - SUMS :] + other[other.shape[0] - SUMS :]


def finish_body(count, coords, mine, other, sums, out, norms):
    whole = add(sums[k] for k in range(NY))
    norms[...] = jnp.sqrt(whole)
    norm = jnp.sqrt(whole / count + EPS)[2:3, :1]
    half = out.shape[1] // 2
    out[0, pl.ds(pl.multiple_of(coords[1] * half, half), half), :] = mine[:half] / norm
    out[0, pl.ds(pl.multiple_of((1 - coords[1]) * half, half), half), :] = other[:half] / norm


def spread(block):
    quarter = block.shape[0] // 2
    a, b = block[:quarter], block[quarter:]
    across = jnp.stack([a] + [shift_by(a, "x", k) for k in (1, 2, 3)])
    along = jnp.stack([b] + [shift_by(b, "y", k) for k in (1, 2, 3)])
    pieces = [across] + [shift_by(across, "y", k) for k in (1, 2, 3)]
    pieces += [along] + [shift_by(along, "x", k) for k in (1, 2, 3)]
    return pieces + [shift_by(piece, "c", 1) for piece in pieces]


def per_device(wavefunction, left_env, right_env, in_sector, out_sector, precond, shifts):
    y, x, z, c = (lax.axis_index(name) for name in AXES)
    coords = jnp.stack([z, c, y, x]).astype(jnp.int32)
    _, size, cols = wavefunction.shape
    half, rows = size // 2, size // 2 // NZ
    count = NY * NX * size * cols
    envs = split_env(left_env, right_env, coords)

    mine = lax.dynamic_slice_in_dim(wavefunction[0], c * half, half, 0)
    own, peer, _ = apply_tasks(spread(mine), envs, in_sector, out_sector, coords)
    updated, sums = local(
        functools.partial(first_update_body, half),
        "first_update",
        [f32(rows, cols), f32(SUMS, cols)],
        [SMEM, SMEM] + [VMEM] * 3,
        [coords, shifts, wavefunction, precond, reduce_to_piece(own, peer, coords)],
    )
    mine = lax.all_gather(updated, "z", axis=0, tiled=True)
    own, peer, square = apply_tasks(spread(mine), envs, in_sector, out_sector, coords)
    (piece,) = local(
        functools.partial(second_update_body, half, count),
        "second_update",
        [f32(rows + SUMS, cols)],
        [SMEM, SMEM] + [VMEM] * 5,
        [coords, shifts, square, updated, sums, precond, reduce_to_piece(own, peer, coords)],
    )
    (mine,) = local(
        place_last_body,
        "place_last",
        [f32(half + SUMS, cols)],
        [VMEM],
        [lax.all_gather(piece, "z")],
    )
    other = shift_by(mine, "c", 1)
    (sums,) = local(join_sums_body, "join_sums", [f32(SUMS, cols)], [VMEM] * 2, [mine, other])
    sums = lax.all_gather(sums, "x").sum(axis=0)
    psi, norms = local(
        functools.partial(finish_body, count),
        "finish",
        [f32(1, size, cols), f32(SUMS, cols)],
        [SMEM] + [VMEM] * 3,
        [coords, mine, other, lax.all_gather(sums, "y")],
    )
    return psi, norms[:ITERS, 0]


def solution(mesh):
    torus = Mesh(mesh.devices.reshape(NY, NX, NZ, NC), AXES)
    placed = (
        P(SECTOR, None, None),
        P(SECTOR_TERM, None, None),
        P(SECTOR_TERM, None, None),
        P(SECTOR_TERM),
        P(SECTOR_TERM),
        P(SECTOR, None, None),
        P(),
    )
    return jax.shard_map(
        per_device,
        mesh=torus,
        in_specs=placed,
        out_specs=(P(SECTOR, None, None), P()),
        check_vma=False,
    )
```

```python
import functools

import jax
import jax.numpy as jnp
from jax import lax
from jax.experimental import pallas as pl
from jax.experimental.pallas import tpu as pltpu
from jax.sharding import Mesh
from jax.sharding import PartitionSpec as P

ITERS = 2
AXES = ("y", "x", "z", "c")
SECTOR = ("y", "x")
SECTOR_TERM = ("y", "x", "z", "c")
NY, NX, NZ, NC = 4, 4, 8, 2
EPS = 1e-06
SUMS = 8


VMEM = pl.BlockSpec(memory_space=pltpu.VMEM)
SMEM = pl.BlockSpec(memory_space=pltpu.SMEM)
HBM = pl.BlockSpec(memory_space=pltpu.HBM)


def f32(*shape):
    return jax.ShapeDtypeStruct(shape, jnp.float32)


def local(body, outs, in_specs, args, scratch=(), flops=0, limit=16 << 20):
    moved = sum(4 * a.size for a in args) + sum(4 * o.size for o in outs)
    return pl.pallas_call(
        body,
        out_shape=tuple(outs),
        in_specs=in_specs,
        out_specs=tuple(VMEM for _ in outs),
        scratch_shapes=list(scratch),
        compiler_params=pltpu.CompilerParams(vmem_limit_bytes=limit),
        cost_estimate=pl.CostEstimate(
            flops=max(flops, moved), bytes_accessed=moved, transcendentals=0
        ),
    )(*args)


def shift_by(value, axis, by):
    size = {"y": NY, "x": NX, "z": NZ, "c": NC}[axis]
    return lax.ppermute(value, axis, [(i, (i + by) % size) for i in range(size)])


def split(value):
    high = value.astype(jnp.bfloat16)
    return high, (value - high.astype(jnp.float32)).astype(jnp.bfloat16)


def product(left, right):
    def part(a, b):
        return jnp.dot(a, b, preferred_element_type=jnp.float32)

    return part(left[0], right[0]) + (part(left[1], right[0]) + part(left[0], right[1]))


def split_body(coords, left, right, left_high, left_low, right_high, right_low):
    half = left.shape[1] // 2
    for side in range(2):
        base = jnp.where(side == 0, coords[1], 1 - coords[1]) * half
        rows = left[0, pl.ds(pl.multiple_of(base, half), half), :]
        there = slice(side * half, (side + 1) * half)
        left_high[0, there], left_low[0, there] = split(rows)
    right_high[0], right_low[0] = split(right[0])


def shift_xor(value, axis, by):
    size = {"y": NY, "x": NX, "z": NZ, "c": NC}[axis]
    return lax.ppermute(value, axis, [(i, i ^ by) for i in range(size)])


def split_env(left_env, right_env, coords):
    block = pl.BlockSpec((1, *left_env.shape[1:]), lambda t: (t, 0, 0))
    return pl.pallas_call(
        split_body,
        grid=(left_env.shape[0],),
        out_shape=(jax.ShapeDtypeStruct(left_env.shape, jnp.bfloat16),) * 4,
        in_specs=[SMEM, block, block],
        out_specs=(block,) * 4,
        compiler_params=pltpu.CompilerParams(
            dimension_semantics=("arbitrary",), vmem_limit_bytes=46 << 20
        ),
        cost_estimate=pl.CostEstimate(
            flops=100 * left_env.size, bytes_accessed=16 * left_env.size, transcendentals=0
        ),
        name="split_env",
    )(coords, left_env, right_env)


def tasks_body(tasks, half, coords, source, target, *refs):
    envs, pieces, outs, square, (psi_high, psi_low) = (
        refs[:4],
        refs[4:20],
        refs[20:24],
        refs[24],
        refs[25:],
    )
    left_high, left_low, right_high, right_low = envs
    for out in outs:
        out[...] = jnp.zeros_like(out)
    quarter = half // 2
    squares = jnp.zeros((quarter, psi_high.shape[-1]), jnp.float32)
    for side in range(2):
        base = jnp.where(side == 0, coords[1], 1 - coords[1]) * half
        for k in range(4):
            for part in range(2):
                rows = pl.ds(pl.multiple_of(base + part * quarter, quarter), quarter)
                piece = pieces[side * 8 + part * 4 + k]
                for j in range(4):
                    value = piece[j]
                    up, over = (k, j) if part == 0 else (j, k)
                    slot = lax.rem(coords[2] + NY - up, NY) * NX + lax.rem(coords[3] + NX - over, NX)
                    psi_high[slot, rows, :], psi_low[slot, rows, :] = split(value)
                    squares += value * value
    square[...] = jnp.full(square.shape, jnp.sum(squares), jnp.float32)

    @pl.loop(0, tasks, unroll=2)
    def _(t):
        slot, goal = source[t], target[t]
        middle = product((left_high[t], left_low[t]), (psi_high[slot], psi_low[slot]))
        result = product(split(middle), (right_high[t], right_low[t]))
        for k, out in enumerate(outs):
            out[goal] += result[k * quarter : (k + 1) * quarter]


def apply_tasks(pieces, envs, in_sector, out_sector, coords):
    tasks, rows, cols = envs[0].shape
    half = rows // 2
    return local(
        functools.partial(tasks_body, tasks, half),
        [f32(16, half // 2, cols)] * 4 + [f32(8, 128)],
        [SMEM, SMEM, SMEM] + [VMEM] * 20,
        [coords, in_sector, out_sector, *envs, *pieces],
        scratch=[pltpu.VMEM((16, rows, cols), jnp.bfloat16)] * 2,
        flops=12 * tasks * rows * rows * cols,
        limit=28 << 20,
    )


def add(values):
    return functools.reduce(lambda p, q: p + q, list(values))


def exchange(value, axis):
    return lax.all_to_all(value, axis, split_axis=0, concat_axis=0, tiled=True)


def join_upper_body(coords, own, got, *outs):
    for k in range(NY):
        up = lax.rem(coords[2] + k, NY)
        for j in range(NX):
            outs[k][j] = own[up * NX + j] + got[up * NX + j]


def join_lower_body(coords, own, got, *outs):
    for k in range(NX):
        over = lax.rem(coords[3] + k, NX)
        for j in range(NY):
            outs[k][j] = own[j * NX + over] + got[j * NX + over]


def sum_first_body(coords, which, *refs):
    parts, outs = refs[:4], refs[4:]
    for k in range(4):
        to = lax.rem(coords[which] + k, 4)
        outs[k][...] = add(ref[to] for ref in parts)


def sum_second_body(*refs):
    a, b, out = refs[:4], refs[4:8], refs[8]
    per = NZ // 2
    rows = a[0].shape[0] // per
    for where, parts in ((0, a), (per, b)):
        value = add(ref[...] for ref in parts)
        for k in range(per):
            out[where + k] = value[k * rows : (k + 1) * rows]


def to_owners(body, own, peer, coords, first, second, which):
    _, quarter, cols = own.shape
    got = shift_by(peer, "c", 1)
    parts = local(body, [f32(4, quarter, cols)] * 4, [SMEM] + [VMEM] * 2, [coords, own, got])
    parts = [parts[0]] + [shift_by(parts[k], first, k) for k in (1, 2, 3)]
    parts = local(
        lambda coords, *refs: sum_first_body(coords, which, *refs),
        [f32(quarter, cols)] * 4,
        [SMEM] + [VMEM] * 4,
        [coords, *parts],
    )
    return [parts[0]] + [shift_by(parts[k], second, k) for k in (1, 2, 3)]


def reduce_to_piece(sums, coords):
    own_a, own_b, peer_a, peer_b = sums
    _, quarter, cols = own_a.shape
    a = to_owners(join_upper_body, own_a, peer_a, coords, "y", "x", 3)
    b = to_owners(join_lower_body, own_b, peer_b, coords, "x", "y", 2)
    (rows_of,) = local(sum_second_body, [f32(NZ, 2 * quarter // NZ, cols)], [VMEM] * 8, a + b)
    return exchange(rows_of, "z")


def total(value):
    return jnp.sum(jnp.sum(value, axis=1, keepdims=True), axis=0, keepdims=True)


def own_rows(coords, half, rows):
    return pl.ds(pl.multiple_of(coords[1] * half + coords[0] * rows, rows), rows)


def first_update_body(half, coords, shifts, psi, precond, parts, updated_ref, sums_ref):
    here = own_rows(coords, half, parts.shape[1])
    sigma = add(parts[k] for k in range(NZ))
    shift = shifts[0]
    current = psi[0, here, :]
    residual = sigma - shift * current
    updated = current - residual / (precond[0, here, :] - shift)
    for k in range(NZ):
        updated_ref[k] = updated
    sums_ref[...] = jnp.broadcast_to(total(residual * residual), sums_ref.shape)


def second_update_body(half, count, coords, shifts, square, before, sums, precond, parts, out):
    rows = parts.shape[1]
    here = own_rows(coords, half, rows)
    norm = jnp.sqrt(square[...] / count + EPS)[:1, :1]
    sigma = add(parts[k] for k in range(NZ)) / norm
    shift = shifts[1]
    current = before[0] / norm
    residual = sigma - shift * current
    updated = current - residual / (precond[0, here, :] - shift)
    line = lax.broadcasted_iota(jnp.int32, sums.shape, 0)
    squares = jnp.where(
        line == 0,
        sums[...],
        jnp.where(line == 1, total(residual * residual), total(updated * updated)),
    )
    for k in range(NZ):
        out[k, :rows] = updated
        out[k, rows:] = squares


def place_last_body(pieces, out):
    rows = pieces.shape[1] - SUMS
    for k in range(NZ):
        out[k * rows : (k + 1) * rows] = pieces[k, :rows]
    out[NZ * rows :] = add(pieces[k, rows:] for k in range(NZ))


def join_sums_body(mine, other, out):
    out[...] = mine[mine.shape[0] - SUMS :] + other[other.shape[0] - SUMS :]


def finish_body(count, coords, mine, other, sums, out, norms):
    whole = sums[...]
    norms[...] = jnp.sqrt(whole)
    norm = jnp.sqrt(whole / count + EPS)[2:3, :1]
    half = out.shape[1] // 2
    out[0, pl.ds(pl.multiple_of(coords[1] * half, half), half), :] = mine[:half] / norm
    out[0, pl.ds(pl.multiple_of((1 - coords[1]) * half, half), half), :] = other[:half] / norm


def spread(block):
    quarter = block.shape[0] // 2
    a, b = block[:quarter], block[quarter:]
    across = jnp.stack([a] + [shift_by(a, "x", k) for k in (1, 2, 3)])
    along = jnp.stack([b] + [shift_by(b, "y", k) for k in (1, 2, 3)])
    pieces = [across] + [shift_by(across, "y", k) for k in (1, 2)]
    pieces += [shift_by(across, "y", 3), along]
    pieces += [shift_by(along, "x", 1)]
    pieces += [shift_by(along, "x", k) for k in (2, 3)]
    return pieces + [shift_by(piece, "c", 1) for piece in pieces]


def per_device(wavefunction, left_env, right_env, in_sector, out_sector, precond, shifts):
    y, x, z, c = (lax.axis_index(name) for name in AXES)
    coords = jnp.stack([z, c, y, x]).astype(jnp.int32)
    _, size, cols = wavefunction.shape
    half, rows = size // 2, size // 2 // NZ
    count = NY * NX * size * cols

    mine = lax.dynamic_slice_in_dim(wavefunction[0], c * half, half, 0)
    envs = split_env(left_env, right_env, coords)
    pieces = spread(mine)
    *parts, _ = apply_tasks(pieces, envs, in_sector, out_sector, coords)
    updated, sums = local(
        functools.partial(first_update_body, half),
        [f32(NZ, rows, cols), f32(SUMS, cols)],
        [SMEM, SMEM] + [VMEM] * 3,
        [coords, shifts, wavefunction, precond, reduce_to_piece(parts, coords)],
    )
    mine = exchange(updated, "z").reshape(half, cols)
    *parts, square = apply_tasks(spread(mine), envs, in_sector, out_sector, coords)
    (piece,) = local(
        functools.partial(second_update_body, half, count),
        [f32(NZ, rows + SUMS, cols)],
        [SMEM, SMEM] + [VMEM] * 5,
        [coords, shifts, square, updated, sums, precond, reduce_to_piece(parts, coords)],
    )
    (mine,) = local(place_last_body, [f32(half + SUMS, cols)], [VMEM], [exchange(piece, "z")])
    other = shift_by(mine, "c", 1)
    (sums,) = local(join_sums_body, [f32(SUMS, cols)], [VMEM] * 2, [mine, other])
    for axis, by in (("x", 1), ("x", 2), ("y", 1), ("y", 2)):
        sums = sums + shift_xor(sums, axis, by)
    psi, norms = local(
        functools.partial(finish_body, count),
        [f32(1, size, cols), f32(SUMS, cols)],
        [SMEM] + [VMEM] * 3,
        [coords, mine, other, sums],
    )
    return psi, norms[:ITERS, 0]


def solution(mesh):
    torus = Mesh(mesh.devices.reshape(NY, NX, NZ, NC), AXES)
    placed = (
        P(SECTOR, None, None),
        P(SECTOR_TERM, None, None),
        P(SECTOR_TERM, None, None),
        P(SECTOR_TERM),
        P(SECTOR_TERM),
        P(SECTOR, None, None),
        P(),
    )
    return jax.shard_map(
        per_device,
        mesh=torus,
        in_specs=placed,
        out_specs=(P(SECTOR, None, None), P()),
        check_vma=False,
    )
```

```python
import functools

import jax
import jax.numpy as jnp
from jax import lax
from jax.experimental import pallas as pl
from jax.experimental.pallas import tpu as pltpu
from jax.sharding import Mesh
from jax.sharding import PartitionSpec as P

ITERS = 2
AXES = ("y", "x", "z", "c")
SECTOR = ("y", "x")
SECTOR_TERM = ("y", "x", "z", "c")
NY, NX, NZ, NC = 4, 4, 8, 2
EPS = 1e-06
SUMS = 8


ORDER = (1, 3, 2)

VMEM = pl.BlockSpec(memory_space=pltpu.VMEM)
SMEM = pl.BlockSpec(memory_space=pltpu.SMEM)
HBM = pl.BlockSpec(memory_space=pltpu.HBM)


def f32(*shape):
    return jax.ShapeDtypeStruct(shape, jnp.float32)


def local(body, outs, in_specs, args, scratch=(), flops=0, limit=16 << 20):
    moved = sum(4 * a.size for a in args) + sum(4 * o.size for o in outs)
    return pl.pallas_call(
        body,
        out_shape=tuple(outs),
        in_specs=in_specs,
        out_specs=tuple(VMEM for _ in outs),
        scratch_shapes=list(scratch),
        compiler_params=pltpu.CompilerParams(vmem_limit_bytes=limit),
        cost_estimate=pl.CostEstimate(
            flops=max(flops, moved), bytes_accessed=moved, transcendentals=0
        ),
    )(*args)


def shift_by(value, axis, by):
    size = {"y": NY, "x": NX, "z": NZ, "c": NC}[axis]
    return lax.ppermute(value, axis, [(i, (i + by) % size) for i in range(size)])


def split(value):
    high = value.astype(jnp.bfloat16)
    return high, (value - high.astype(jnp.float32)).astype(jnp.bfloat16)


def product(left, right):
    def part(a, b):
        return jnp.dot(a, b, preferred_element_type=jnp.float32)

    return part(left[0], right[0]) + (part(left[1], right[0]) + part(left[0], right[1]))


def split_body(left, right, left_high, left_low, right_high, right_low):
    half = left.shape[1] // 2
    core = lax.axis_index("c")
    for side in range(2):
        base = (core if side == 0 else 1 - core) * half
        rows = left[0, pl.ds(pl.multiple_of(base, half), half), :]
        there = slice(side * half, (side + 1) * half)
        left_high[0, there], left_low[0, there] = split(rows)
    right_high[0], right_low[0] = split(right[0])


def shift_xor(value, axis, by):
    size = {"y": NY, "x": NX, "z": NZ, "c": NC}[axis]
    return lax.ppermute(value, axis, [(i, i ^ by) for i in range(size)])


def split_env(left_env, right_env):
    block = pl.BlockSpec((1, *left_env.shape[1:]), lambda t: (t, 0, 0))
    return pl.pallas_call(
        split_body,
        grid=(left_env.shape[0],),
        out_shape=(jax.ShapeDtypeStruct(left_env.shape, jnp.bfloat16),) * 4,
        in_specs=[block, block],
        out_specs=(block,) * 4,
        compiler_params=pltpu.CompilerParams(
            dimension_semantics=("arbitrary",), vmem_limit_bytes=46 << 20
        ),
        cost_estimate=pl.CostEstimate(
            flops=100 * left_env.size, bytes_accessed=16 * left_env.size, transcendentals=0
        ),
        name="split_env",
    )(left_env, right_env)


def tasks_body(tasks, half, sectors, *refs):
    envs, pieces, outs, square, (psi_high, psi_low) = (
        refs[:4],
        refs[4:20],
        refs[20:24],
        refs[24],
        refs[25:],
    )
    left_high, left_low, right_high, right_low = envs
    for out in outs:
        out[...] = jnp.zeros_like(out)
    quarter = half // 2
    squares = jnp.zeros((quarter, psi_high.shape[-1]), jnp.float32)
    y, x, core = (lax.axis_index(name) for name in ("y", "x", "c"))
    for side in range(2):
        base = (core if side == 0 else 1 - core) * half
        for k in range(4):
            for part in range(2):
                rows = pl.ds(pl.multiple_of(base + part * quarter, quarter), quarter)
                piece = pieces[side * 8 + part * 4 + k]
                for j in range(4):
                    value = piece[j]
                    up, over = (k, j) if part == 0 else (j, k)
                    slot = lax.rem(y + NY - up, NY) * NX + lax.rem(x + NX - over, NX)
                    psi_high[slot, rows, :], psi_low[slot, rows, :] = split(value)
                    squares += value * value
    square[...] = jnp.full(square.shape, jnp.sum(squares), jnp.float32)

    @pl.loop(0, tasks, unroll=2)
    def _(t):
        slot, goal = sectors[t], sectors[tasks + t]
        middle = product((left_high[t], left_low[t]), (psi_high[slot], psi_low[slot]))
        result = product(split(middle), (right_high[t], right_low[t]))
        for k, out in enumerate(outs):
            out[goal] += result[k * quarter : (k + 1) * quarter]


def apply_tasks(pieces, envs, sectors):
    tasks, rows, cols = envs[0].shape
    half = rows // 2
    return local(
        functools.partial(tasks_body, tasks, half),
        [f32(16, half // 2, cols)] * 4 + [f32(8, 128)],
        [SMEM] + [VMEM] * 20,
        [sectors, *envs, *pieces],
        scratch=[pltpu.VMEM((16, rows, cols), jnp.bfloat16)] * 2,
        flops=12 * tasks * rows * rows * cols,
        limit=28 << 20,
    )


def add(values):
    return functools.reduce(lambda p, q: p + q, list(values))


def exchange(value, axis):
    return lax.all_to_all(value, axis, split_axis=0, concat_axis=0, tiled=True)


def join_upper_body(own, got, *outs):
    for k in range(NY):
        up = lax.rem(lax.axis_index("y") + k, NY)
        for j in range(NX):
            outs[k][j] = own[up * NX + j] + got[up * NX + j]


def join_lower_body(own, got, *outs):
    for k in range(NX):
        over = lax.rem(lax.axis_index("x") + k, NX)
        for j in range(NY):
            outs[k][j] = own[j * NX + over] + got[j * NX + over]


def sum_first_body(axis, *refs):
    parts, outs = refs[:4], refs[4:]
    for k in range(4):
        to = lax.rem(lax.axis_index(axis) + k, 4)
        outs[k][...] = add(ref[to] for ref in parts)


def sum_second_body(*refs):
    a, b, out = refs[:4], refs[4:8], refs[8]
    per = NZ // 2
    rows = a[0].shape[0] // per
    for where, parts in ((0, a), (per, b)):
        value = add(ref[...] for ref in parts)
        for k in range(per):
            out[where + k] = value[k * rows : (k + 1) * rows]


def to_owners(body, own, peer, first, second):
    _, quarter, cols = own.shape
    got = shift_by(peer, "c", 1)
    parts = local(body, [f32(4, quarter, cols)] * 4, [VMEM] * 2, [own, got])
    parts = [parts[0]] + [shift_by(parts[k], first, k) for k in ORDER]
    parts = local(
        functools.partial(sum_first_body, second), [f32(quarter, cols)] * 4, [VMEM] * 4, parts
    )
    return [parts[0]] + [shift_by(parts[k], second, k) for k in ORDER]


def reduce_to_piece(sums):
    own_a, own_b, peer_a, peer_b = sums
    _, quarter, cols = own_a.shape
    a = to_owners(join_upper_body, own_a, peer_a, "y", "x")
    b = to_owners(join_lower_body, own_b, peer_b, "x", "y")
    (rows_of,) = local(sum_second_body, [f32(NZ, 2 * quarter // NZ, cols)], [VMEM] * 8, a + b)
    return exchange(rows_of, "z")


def total(value):
    return jnp.sum(jnp.sum(value, axis=1, keepdims=True), axis=0, keepdims=True)


def own_rows(half, rows):
    start = lax.axis_index("c") * half + lax.axis_index("z") * rows
    return pl.ds(pl.multiple_of(start, rows), rows)


def first_update_body(half, shifts, psi, precond, parts, updated_ref, sums_ref):
    here = own_rows(half, parts.shape[1])
    sigma = add(parts[k] for k in range(NZ))
    shift = shifts[:1, :1]
    current = psi[0, here, :]
    residual = sigma - shift * current
    updated = current - residual / (precond[0, here, :] - shift)
    for k in range(NZ):
        updated_ref[k] = updated
    sums_ref[...] = jnp.broadcast_to(total(residual * residual), sums_ref.shape)


def second_update_body(half, count, shifts, square, before, sums, precond, parts, out):
    rows = parts.shape[1]
    here = own_rows(half, rows)
    norm = jnp.sqrt(square[...] / count + EPS)[:1, :1]
    sigma = add(parts[k] for k in range(NZ)) / norm
    shift = shifts[1:2, :1]
    current = before[0] / norm
    residual = sigma - shift * current
    updated = current - residual / (precond[0, here, :] - shift)
    line = lax.broadcasted_iota(jnp.int32, sums.shape, 0)
    squares = jnp.where(
        line == 0,
        sums[...],
        jnp.where(line == 1, total(residual * residual), total(updated * updated)),
    )
    for k in range(NZ):
        out[k, :rows] = updated
        out[k, rows:] = squares


def place_last_body(pieces, out):
    rows = pieces.shape[1] - SUMS
    for k in range(NZ):
        out[k * rows : (k + 1) * rows] = pieces[k, :rows]
    out[NZ * rows :] = add(pieces[k, rows:] for k in range(NZ))


def join_sums_body(mine, other, out):
    out[...] = mine[mine.shape[0] - SUMS :] + other[other.shape[0] - SUMS :]


def finish_body(count, mine, other, sums, out, norms):
    whole = sums[...]
    norms[...] = jnp.sqrt(whole)
    norm = jnp.sqrt(whole / count + EPS)[2:3, :1]
    half = out.shape[1] // 2
    core = lax.axis_index("c")
    out[0, pl.ds(pl.multiple_of(core * half, half), half), :] = mine[:half] / norm
    out[0, pl.ds(pl.multiple_of((1 - core) * half, half), half), :] = other[:half] / norm


def spread(block):
    quarter = block.shape[0] // 2
    a, b = block[:quarter], block[quarter:]
    across = jnp.stack([a] + [shift_by(a, "x", k) for k in (1, 2, 3)])
    along = jnp.stack([b] + [shift_by(b, "y", k) for k in (1, 2, 3)])
    pieces = [across] + [shift_by(across, "y", k) for k in (1, 2)]
    pieces += [shift_by(across, "y", 3), along]
    pieces += [shift_by(along, "x", 1)]
    pieces += [shift_by(along, "x", k) for k in (2, 3)]
    return pieces + [shift_by(piece, "c", 1) for piece in pieces]


def per_device(wavefunction, left_env, right_env, in_sector, out_sector, precond, shifts):
    sectors = jnp.concatenate([in_sector, out_sector])
    shifts = jnp.broadcast_to(shifts[:, None], (ITERS, 128))
    _, size, cols = wavefunction.shape
    half, rows = size // 2, size // 2 // NZ
    count = NY * NX * size * cols

    mine = lax.dynamic_slice_in_dim(wavefunction[0], lax.axis_index("c") * half, half, 0)
    envs = split_env(left_env, right_env)
    pieces = spread(mine)
    *parts, _ = apply_tasks(pieces, envs, sectors)
    updated, sums = local(
        functools.partial(first_update_body, half),
        [f32(NZ, rows, cols), f32(SUMS, cols)],
        [VMEM] * 4,
        [shifts, wavefunction, precond, reduce_to_piece(parts)],
    )
    mine = exchange(updated, "z").reshape(half, cols)
    *parts, square = apply_tasks(spread(mine), envs, sectors)
    (piece,) = local(
        functools.partial(second_update_body, half, count),
        [f32(NZ, rows + SUMS, cols)],
        [VMEM] * 6,
        [shifts, square, updated, sums, precond, reduce_to_piece(parts)],
    )
    (mine,) = local(place_last_body, [f32(half + SUMS, cols)], [VMEM], [exchange(piece, "z")])
    other = shift_by(mine, "c", 1)
    (sums,) = local(join_sums_body, [f32(SUMS, cols)], [VMEM] * 2, [mine, other])
    for axis, by in (("x", 1), ("x", 2), ("y", 1), ("y", 2)):
        sums = sums + shift_xor(sums, axis, by)
    psi, norms = local(
        functools.partial(finish_body, count),
        [f32(1, size, cols), f32(SUMS, cols)],
        [VMEM] * 3,
        [mine, other, sums],
    )
    return psi, norms[:ITERS, 0]


def solution(mesh):
    torus = Mesh(mesh.devices.reshape(NY, NX, NZ, NC), AXES)
    placed = (
        P(SECTOR, None, None),
        P(SECTOR_TERM, None, None),
        P(SECTOR_TERM, None, None),
        P(SECTOR_TERM),
        P(SECTOR_TERM),
        P(SECTOR, None, None),
        P(),
    )
    return jax.shard_map(
        per_device,
        mesh=torus,
        in_specs=placed,
        out_specs=(P(SECTOR, None, None), P()),
        check_vma=False,
    )
```

```python
import functools

import jax
import jax.numpy as jnp
from jax import lax
from jax.experimental import pallas as pl
from jax.experimental.pallas import tpu as pltpu
from jax.sharding import Mesh
from jax.sharding import PartitionSpec as P

ITERS = 2
AXES = ("y", "x", "z", "c")
SECTOR = ("y", "x")
SECTOR_TERM = ("y", "x", "z", "c")
NY, NX, NZ, NC = 4, 4, 8, 2
EPS = 1e-06
SUMS = 8


ORDER = (1, 3, 2)

VMEM = pl.BlockSpec(memory_space=pltpu.VMEM)
SMEM = pl.BlockSpec(memory_space=pltpu.SMEM)
HBM = pl.BlockSpec(memory_space=pltpu.HBM)


def f32(*shape):
    return jax.ShapeDtypeStruct(shape, jnp.float32)


def local(body, outs, in_specs, args, scratch=(), flops=0, limit=16 << 20):
    moved = sum(4 * a.size for a in args) + sum(4 * o.size for o in outs)
    return pl.pallas_call(
        body,
        out_shape=tuple(outs),
        in_specs=in_specs,
        out_specs=tuple(VMEM for _ in outs),
        scratch_shapes=list(scratch),
        compiler_params=pltpu.CompilerParams(vmem_limit_bytes=limit),
        cost_estimate=pl.CostEstimate(
            flops=max(flops, moved), bytes_accessed=moved, transcendentals=0
        ),
    )(*args)


def shift_by(value, axis, by):
    size = {"y": NY, "x": NX, "z": NZ, "c": NC}[axis]
    return lax.ppermute(value, axis, [(i, (i + by) % size) for i in range(size)])


def split(value):
    high = value.astype(jnp.bfloat16)
    return high, (value - high.astype(jnp.float32)).astype(jnp.bfloat16)


def product(left, right):
    def part(a, b):
        return jnp.dot(a, b, preferred_element_type=jnp.float32)

    return part(left[0], right[0]) + (part(left[1], right[0]) + part(left[0], right[1]))


def split_body(left, right, left_high, left_low, right_high, right_low):
    half = left.shape[1] // 2
    core = lax.axis_index("c")
    for side in range(2):
        base = (core if side == 0 else 1 - core) * half
        rows = left[0, pl.ds(pl.multiple_of(base, half), half), :]
        there = slice(side * half, (side + 1) * half)
        left_high[0, there], left_low[0, there] = split(rows)
    right_high[0], right_low[0] = split(right[0])


def split_env(left_env, right_env):
    block = pl.BlockSpec((1, *left_env.shape[1:]), lambda t: (t, 0, 0))
    return pl.pallas_call(
        split_body,
        grid=(left_env.shape[0],),
        out_shape=(jax.ShapeDtypeStruct(left_env.shape, jnp.bfloat16),) * 4,
        in_specs=[block, block],
        out_specs=(block,) * 4,
        compiler_params=pltpu.CompilerParams(
            dimension_semantics=("arbitrary",), vmem_limit_bytes=46 << 20
        ),
        cost_estimate=pl.CostEstimate(
            flops=100 * left_env.size, bytes_accessed=16 * left_env.size, transcendentals=0
        ),
        name="split_env",
    )(left_env, right_env)


def tasks_body(tasks, half, sectors, *refs):
    envs, pieces, outs, square, (psi_high, psi_low) = (
        refs[:4],
        refs[4:12],
        refs[12:16],
        refs[16],
        refs[17:],
    )
    left_high, left_low, right_high, right_low = envs
    for out in outs:
        out[...] = jnp.zeros_like(out)
    quarter = half // 2
    squares = jnp.zeros((quarter, psi_high.shape[-1]), jnp.float32)
    y, x, core = (lax.axis_index(name) for name in ("y", "x", "c"))
    for side in range(2):
        base = (core if side == 0 else 1 - core) * half
        for k in range(4):
            for part in range(2):
                rows = pl.ds(pl.multiple_of(base + part * quarter, quarter), quarter)
                near, far = pieces[side * 4 + part * 2 : side * 4 + part * 2 + 2]
                for j in range(4):
                    value = near[j] if k == 0 else far[k - 1, j]
                    up, over = (k, j) if part == 0 else (j, k)
                    slot = lax.rem(y + NY - up, NY) * NX + lax.rem(x + NX - over, NX)
                    psi_high[slot, rows, :], psi_low[slot, rows, :] = split(value)
                    squares += value * value
    square[...] = jnp.full(square.shape, jnp.sum(squares), jnp.float32)

    @pl.loop(0, tasks, unroll=2)
    def _(t):
        slot, goal = sectors[t], sectors[tasks + t]
        middle = product((left_high[t], left_low[t]), (psi_high[slot], psi_low[slot]))
        result = product(split(middle), (right_high[t], right_low[t]))
        for k, out in enumerate(outs):
            out[goal] += result[k * quarter : (k + 1) * quarter]


def apply_tasks(pieces, envs, sectors):
    tasks, rows, cols = envs[0].shape
    half = rows // 2
    return local(
        functools.partial(tasks_body, tasks, half),
        [f32(16, half // 2, cols)] * 4 + [f32(8, 128)],
        [SMEM] + [VMEM] * 12,
        [sectors, *envs, *pieces],
        scratch=[pltpu.VMEM((16, rows, cols), jnp.bfloat16)] * 2,
        flops=12 * tasks * rows * rows * cols,
        limit=28 << 20,
    )


def add(values):
    return functools.reduce(lambda p, q: p + q, list(values))


def exchange(value, axis):
    return lax.all_to_all(value, axis, split_axis=0, concat_axis=0, tiled=True)


def join_upper_body(own, got, *outs):
    for k in range(NY):
        up = lax.rem(lax.axis_index("y") + k, NY)
        for j in range(NX):
            outs[k][j] = own[up * NX + j] + got[up * NX + j]


def join_lower_body(own, got, *outs):
    for k in range(NX):
        over = lax.rem(lax.axis_index("x") + k, NX)
        for j in range(NY):
            outs[k][j] = own[j * NX + over] + got[j * NX + over]


def sum_first_body(axis, *refs):
    parts, outs = refs[:4], refs[4:]
    for k in range(4):
        to = lax.rem(lax.axis_index(axis) + k, 4)
        outs[k][...] = add(ref[to] for ref in parts)


def sum_second_body(*refs):
    a, b, out = refs[:4], refs[4:8], refs[8]
    per = NZ // 2
    rows = a[0].shape[0] // per
    for where, parts in ((0, a), (per, b)):
        value = add(ref[...] for ref in parts)
        for k in range(per):
            out[where + k] = value[k * rows : (k + 1) * rows]


def to_owners(body, own, peer, first, second):
    _, quarter, cols = own.shape
    got = shift_by(peer, "c", 1)
    parts = local(body, [f32(4, quarter, cols)] * 4, [VMEM] * 2, [own, got])
    parts = [parts[0]] + [shift_by(parts[k], first, k) for k in ORDER]
    parts = local(
        functools.partial(sum_first_body, second), [f32(quarter, cols)] * 4, [VMEM] * 4, parts
    )
    return [parts[0]] + [shift_by(parts[k], second, k) for k in ORDER]


def reduce_to_piece(sums):
    own_a, own_b, peer_a, peer_b = sums
    _, quarter, cols = own_a.shape
    a = to_owners(join_upper_body, own_a, peer_a, "y", "x")
    b = to_owners(join_lower_body, own_b, peer_b, "x", "y")
    (rows_of,) = local(sum_second_body, [f32(NZ, 2 * quarter // NZ, cols)], [VMEM] * 8, a + b)
    return exchange(rows_of, "z")


def total(value):
    return jnp.sum(jnp.sum(value, axis=1, keepdims=True), axis=0, keepdims=True)


def own_rows(half, rows):
    start = lax.axis_index("c") * half + lax.axis_index("z") * rows
    return pl.ds(pl.multiple_of(start, rows), rows)


def first_update_body(half, shifts, psi, precond, parts, updated_ref, sums_ref):
    here = own_rows(half, parts.shape[1])
    sigma = add(parts[k] for k in range(NZ))
    shift = shifts[:1, :1]
    current = psi[0, here, :]
    residual = sigma - shift * current
    updated = current - residual / (precond[0, here, :] - shift)
    for k in range(NZ):
        updated_ref[k] = updated
    sums_ref[...] = jnp.broadcast_to(total(residual * residual), sums_ref.shape)


def second_update_body(half, count, shifts, square, before, sums, precond, parts, out):
    rows = parts.shape[1]
    here = own_rows(half, rows)
    norm = jnp.sqrt(square[...] / count + EPS)[:1, :1]
    sigma = add(parts[k] for k in range(NZ)) / norm
    shift = shifts[1:2, :1]
    current = before[0] / norm
    residual = sigma - shift * current
    updated = current - residual / (precond[0, here, :] - shift)
    line = lax.broadcasted_iota(jnp.int32, sums.shape, 0)
    squares = jnp.where(
        line == 0,
        sums[...],
        jnp.where(line == 1, total(residual * residual), total(updated * updated)),
    )
    for k in range(NZ):
        out[k, :rows] = updated
        out[k, rows:] = squares


def place_last_body(pieces, out):
    rows = pieces.shape[1] - SUMS
    for k in range(NZ):
        out[k * rows : (k + 1) * rows] = pieces[k, :rows]
    out[NZ * rows :] = add(pieces[k, rows:] for k in range(NZ))


def join_sums_body(mine, other, out):
    out[...] = mine[mine.shape[0] - SUMS :] + other[other.shape[0] - SUMS :]


def finish_body(count, mine, other, sums, out, norms):
    whole = sums[...]
    norms[...] = jnp.sqrt(whole)
    norm = jnp.sqrt(whole / count + EPS)[2:3, :1]
    half = out.shape[1] // 2
    core = lax.axis_index("c")
    out[0, pl.ds(pl.multiple_of(core * half, half), half), :] = mine[:half] / norm
    out[0, pl.ds(pl.multiple_of((1 - core) * half, half), half), :] = other[:half] / norm


def fan(value, axis):
    got = {k: shift_by(value, axis, k) for k in (2, 1, 3)}
    return [got[k] for k in (1, 2, 3)]


def spread(block):
    quarter = block.shape[0] // 2
    a, b = block[:quarter], block[quarter:]
    across = jnp.stack([a] + fan(a, "x"))
    along = jnp.stack([b] + fan(b, "y"))
    far_a, far_b = fan(across, "y"), fan(along, "x")
    other_a, other_b = shift_by(across, "c", 1), shift_by(along, "c", 1)
    far_a, far_b = jnp.stack(far_a), jnp.stack(far_b)
    others = [other_a, shift_by(far_a, "c", 1), other_b, shift_by(far_b, "c", 1)]
    return [across, far_a, along, far_b] + others


def per_device(wavefunction, left_env, right_env, in_sector, out_sector, precond, shifts):
    sectors = jnp.concatenate([in_sector, out_sector])
    shifts = jnp.broadcast_to(shifts[:, None], (ITERS, 128))
    _, size, cols = wavefunction.shape
    half, rows = size // 2, size // 2 // NZ
    count = NY * NX * size * cols

    mine = lax.dynamic_slice_in_dim(wavefunction[0], lax.axis_index("c") * half, half, 0)
    envs = split_env(left_env, right_env)
    pieces = spread(mine)
    *parts, _ = apply_tasks(pieces, envs, sectors)
    updated, sums = local(
        functools.partial(first_update_body, half),
        [f32(NZ, rows, cols), f32(SUMS, cols)],
        [VMEM] * 4,
        [shifts, wavefunction, precond, reduce_to_piece(parts)],
    )
    mine = exchange(updated, "z").reshape(half, cols)
    pieces = spread(mine)
    *parts, square = apply_tasks(pieces, envs, sectors)
    (piece,) = local(
        functools.partial(second_update_body, half, count),
        [f32(NZ, rows + SUMS, cols)],
        [VMEM] * 6,
        [shifts, square, updated, sums, precond, reduce_to_piece(parts)],
    )
    (mine,) = local(place_last_body, [f32(half + SUMS, cols)], [VMEM], [exchange(piece, "z")])
    other = shift_by(mine, "c", 1)
    (sums,) = local(join_sums_body, [f32(SUMS, cols)], [VMEM] * 2, [mine, other])
    for axis in ("x", "y"):
        one, three, two = (shift_by(sums, axis, k) for k in ORDER)
        sums = (sums + two) + (one + three)
    psi, norms = local(
        functools.partial(finish_body, count),
        [f32(1, size, cols), f32(SUMS, cols)],
        [VMEM] * 3,
        [mine, other, sums],
    )
    return psi, norms[:ITERS, 0]


def solution(mesh):
    torus = Mesh(mesh.devices.reshape(NY, NX, NZ, NC), AXES)
    placed = (
        P(SECTOR, None, None),
        P(SECTOR_TERM, None, None),
        P(SECTOR_TERM, None, None),
        P(SECTOR_TERM),
        P(SECTOR_TERM),
        P(SECTOR, None, None),
        P(),
    )
    return jax.shard_map(
        per_device,
        mesh=torus,
        in_specs=placed,
        out_specs=(P(SECTOR, None, None), P()),
        check_vma=False,
    )
```

```python
import functools

import jax
import jax.numpy as jnp
from jax import lax
from jax.experimental import pallas as pl
from jax.experimental.pallas import tpu as pltpu
from jax.sharding import Mesh
from jax.sharding import PartitionSpec as P

ITERS = 2
AXES = ("y", "x", "z", "c")
SECTOR = ("y", "x")
SECTOR_TERM = ("y", "x", "z", "c")
NY, NX, NZ, NC = 4, 4, 8, 2
EPS = 1e-06
SUMS = 8


ORDER = (1, 3, 2)

VMEM = pl.BlockSpec(memory_space=pltpu.VMEM)
SMEM = pl.BlockSpec(memory_space=pltpu.SMEM)
HBM = pl.BlockSpec(memory_space=pltpu.HBM)


def f32(*shape):
    return jax.ShapeDtypeStruct(shape, jnp.float32)


def local(body, outs, in_specs, args, scratch=(), flops=0, limit=16 << 20):
    moved = sum(4 * a.size for a in args) + sum(4 * o.size for o in outs)
    return pl.pallas_call(
        body,
        out_shape=tuple(outs),
        in_specs=in_specs,
        out_specs=tuple(VMEM for _ in outs),
        scratch_shapes=list(scratch),
        compiler_params=pltpu.CompilerParams(vmem_limit_bytes=limit),
        cost_estimate=pl.CostEstimate(
            flops=max(flops, moved), bytes_accessed=moved, transcendentals=0
        ),
    )(*args)


def shift_by(value, axis, by):
    size = {"y": NY, "x": NX, "z": NZ, "c": NC}[axis]
    return lax.ppermute(value, axis, [(i, (i + by) % size) for i in range(size)])


def split(value):
    high = value.astype(jnp.bfloat16)
    return high, (value - high.astype(jnp.float32)).astype(jnp.bfloat16)


def product(left, right):
    def part(a, b):
        return jnp.dot(a, b, preferred_element_type=jnp.float32)

    return part(left[0], right[0]) + (part(left[1], right[0]) + part(left[0], right[1]))


def split_body(left, right, left_high, left_low, right_high, right_low):
    half = left.shape[1] // 2
    core = lax.axis_index("c")
    for side in range(2):
        base = (core if side == 0 else 1 - core) * half
        rows = left[0, pl.ds(pl.multiple_of(base, half), half), :]
        there = slice(side * half, (side + 1) * half)
        left_high[0, there], left_low[0, there] = split(rows)
    right_high[0], right_low[0] = split(right[0])


def split_env(left_env, right_env):
    block = pl.BlockSpec((1, *left_env.shape[1:]), lambda t: (t, 0, 0))
    return pl.pallas_call(
        split_body,
        grid=(left_env.shape[0],),
        out_shape=(jax.ShapeDtypeStruct(left_env.shape, jnp.bfloat16),) * 4,
        in_specs=[block, block],
        out_specs=(block,) * 4,
        compiler_params=pltpu.CompilerParams(
            dimension_semantics=("arbitrary",), vmem_limit_bytes=46 << 20
        ),
        cost_estimate=pl.CostEstimate(
            flops=100 * left_env.size, bytes_accessed=16 * left_env.size, transcendentals=0
        ),
        name="split_env",
    )(left_env, right_env)


def tasks_body(tasks, half, sectors, *refs):
    envs, pieces, outs, square, (psi_high, psi_low) = (
        refs[:4],
        refs[4:20],
        refs[20:24],
        refs[24],
        refs[25:],
    )
    left_high, left_low, right_high, right_low = envs
    for out in outs:
        out[...] = jnp.zeros_like(out)
    quarter = half // 2
    squares = jnp.zeros((quarter, psi_high.shape[-1]), jnp.float32)
    y, x, core = (lax.axis_index(name) for name in ("y", "x", "c"))
    for side in range(2):
        base = (core if side == 0 else 1 - core) * half
        for k in range(4):
            for part in range(2):
                rows = pl.ds(pl.multiple_of(base + part * quarter, quarter), quarter)
                piece = pieces[side * 8 + part * 4 + k]
                for j in range(4):
                    value = piece[j]
                    up, over = (k, j) if part == 0 else (j, k)
                    slot = lax.rem(y + NY - up, NY) * NX + lax.rem(x + NX - over, NX)
                    psi_high[slot, rows, :], psi_low[slot, rows, :] = split(value)
                    squares += value * value
    square[...] = jnp.full(square.shape, jnp.sum(squares), jnp.float32)

    @pl.loop(0, tasks, unroll=3)
    def _(t):
        slot, goal = sectors[t], sectors[tasks + t]
        middle = product((left_high[t], left_low[t]), (psi_high[slot], psi_low[slot]))
        result = product(split(middle), (right_high[t], right_low[t]))
        for k, out in enumerate(outs):
            out[goal] += result[k * quarter : (k + 1) * quarter]


def apply_tasks(pieces, envs, sectors):
    tasks, rows, cols = envs[0].shape
    half = rows // 2
    return local(
        functools.partial(tasks_body, tasks, half),
        [f32(16, half // 2, cols)] * 4 + [f32(8, 128)],
        [SMEM] + [VMEM] * 20,
        [sectors, *envs, *pieces],
        scratch=[pltpu.VMEM((16, rows, cols), jnp.bfloat16)] * 2,
        flops=12 * tasks * rows * rows * cols,
        limit=28 << 20,
    )


def add(values):
    return functools.reduce(lambda p, q: p + q, list(values))


def exchange(value, axis):
    return lax.all_to_all(value, axis, split_axis=0, concat_axis=0, tiled=True)


def join_upper_body(own, got, *outs):
    for k in range(NY):
        up = lax.rem(lax.axis_index("y") + k, NY)
        for j in range(NX):
            outs[k][j] = own[up * NX + j] + got[up * NX + j]


def join_lower_body(own, got, *outs):
    for k in range(NX):
        over = lax.rem(lax.axis_index("x") + k, NX)
        for j in range(NY):
            outs[k][j] = own[j * NX + over] + got[j * NX + over]


def sum_first_body(axis, *refs):
    parts, outs = refs[:4], refs[4:]
    for k in range(4):
        to = lax.rem(lax.axis_index(axis) + k, 4)
        outs[k][...] = add(ref[to] for ref in parts)


def sum_second_body(*refs):
    a, b, out = refs[:4], refs[4:8], refs[8]
    per = NZ // 2
    rows = a[0].shape[0] // per
    for where, parts in ((0, a), (per, b)):
        value = add(ref[...] for ref in parts)
        for k in range(per):
            out[where + k] = value[k * rows : (k + 1) * rows]


def to_owners(body, own, peer, first, second):
    _, quarter, cols = own.shape
    got = shift_by(peer, "c", 1)
    parts = local(body, [f32(4, quarter, cols)] * 4, [VMEM] * 2, [own, got])
    parts = [parts[0]] + [shift_by(parts[k], first, k) for k in ORDER]
    parts = local(
        functools.partial(sum_first_body, second), [f32(quarter, cols)] * 4, [VMEM] * 4, parts
    )
    return [parts[0]] + [shift_by(parts[k], second, k) for k in ORDER]


def reduce_to_piece(sums):
    own_a, own_b, peer_a, peer_b = sums
    _, quarter, cols = own_a.shape
    a = to_owners(join_upper_body, own_a, peer_a, "y", "x")
    b = to_owners(join_lower_body, own_b, peer_b, "x", "y")
    (rows_of,) = local(sum_second_body, [f32(NZ, 2 * quarter // NZ, cols)], [VMEM] * 8, a + b)
    return exchange(rows_of, "z")


def total(value):
    return jnp.sum(jnp.sum(value, axis=1, keepdims=True), axis=0, keepdims=True)


def own_rows(half, rows):
    start = lax.axis_index("c") * half + lax.axis_index("z") * rows
    return pl.ds(pl.multiple_of(start, rows), rows)


def first_update_body(half, shifts, psi, precond, parts, updated_ref, sums_ref):
    here = own_rows(half, parts.shape[1])
    sigma = add(parts[k] for k in range(NZ))
    shift = shifts[:1, :1]
    current = psi[0, here, :]
    residual = sigma - shift * current
    updated = current - residual / (precond[0, here, :] - shift)
    for k in range(NZ):
        updated_ref[k] = updated
    sums_ref[...] = jnp.broadcast_to(total(residual * residual), sums_ref.shape)


def second_update_body(half, count, shifts, square, before, sums, precond, parts, out):
    rows = parts.shape[1]
    here = own_rows(half, rows)
    norm = jnp.sqrt(square[...] / count + EPS)[:1, :1]
    sigma = add(parts[k] for k in range(NZ)) / norm
    shift = shifts[1:2, :1]
    current = before[0] / norm
    residual = sigma - shift * current
    updated = current - residual / (precond[0, here, :] - shift)
    line = lax.broadcasted_iota(jnp.int32, sums.shape, 0)
    squares = jnp.where(
        line == 0,
        sums[...],
        jnp.where(line == 1, total(residual * residual), total(updated * updated)),
    )
    for k in range(NZ):
        out[k, :rows] = updated
        out[k, rows:] = squares


def place_last_body(pieces, out):
    rows = pieces.shape[1] - SUMS
    for k in range(NZ):
        out[k * rows : (k + 1) * rows] = pieces[k, :rows]
    out[NZ * rows :] = add(pieces[k, rows:] for k in range(NZ))


def join_sums_body(mine, other, out):
    out[...] = mine[mine.shape[0] - SUMS :] + other[other.shape[0] - SUMS :]


def finish_body(count, mine, other, sums, out, norms):
    whole = sums[...]
    norms[...] = jnp.sqrt(whole)
    norm = jnp.sqrt(whole / count + EPS)[2:3, :1]
    half = out.shape[1] // 2
    core = lax.axis_index("c")
    out[0, pl.ds(pl.multiple_of(core * half, half), half), :] = mine[:half] / norm
    out[0, pl.ds(pl.multiple_of((1 - core) * half, half), half), :] = other[:half] / norm


def spread(block):
    quarter = block.shape[0] // 2
    a, b = block[:quarter], block[quarter:]
    across = jnp.stack([a] + [shift_by(a, "x", k) for k in (1, 2, 3)])
    along = jnp.stack([b] + [shift_by(b, "y", k) for k in (1, 2, 3)])
    pieces = [across] + [shift_by(across, "y", k) for k in (1, 2)]
    pieces += [shift_by(across, "y", 3), along]
    pieces += [shift_by(along, "x", 1)]
    pieces += [shift_by(along, "x", k) for k in (2, 3)]
    return pieces + [shift_by(piece, "c", 1) for piece in pieces]


def per_device(wavefunction, left_env, right_env, in_sector, out_sector, precond, shifts):
    sectors = jnp.concatenate([in_sector, out_sector])
    shifts = jnp.broadcast_to(shifts[:, None], (ITERS, 128))
    _, size, cols = wavefunction.shape
    half, rows = size // 2, size // 2 // NZ
    count = NY * NX * size * cols

    mine = lax.dynamic_slice_in_dim(wavefunction[0], lax.axis_index("c") * half, half, 0)
    envs = split_env(left_env, right_env)
    pieces = spread(mine)
    *parts, _ = apply_tasks(pieces, envs, sectors)
    updated, sums = local(
        functools.partial(first_update_body, half),
        [f32(NZ, rows, cols), f32(SUMS, cols)],
        [VMEM] * 4,
        [shifts, wavefunction, precond, reduce_to_piece(parts)],
    )
    mine = exchange(updated, "z").reshape(half, cols)
    *parts, square = apply_tasks(spread(mine), envs, sectors)
    (piece,) = local(
        functools.partial(second_update_body, half, count),
        [f32(NZ, rows + SUMS, cols)],
        [VMEM] * 6,
        [shifts, square, updated, sums, precond, reduce_to_piece(parts)],
    )
    (mine,) = local(place_last_body, [f32(half + SUMS, cols)], [VMEM], [exchange(piece, "z")])
    other = shift_by(mine, "c", 1)
    (sums,) = local(join_sums_body, [f32(SUMS, cols)], [VMEM] * 2, [mine, other])
    for axis in ("x", "y"):
        one, three, two = (shift_by(sums, axis, k) for k in ORDER)
        sums = (sums + two) + (one + three)
    psi, norms = local(
        functools.partial(finish_body, count),
        [f32(1, size, cols), f32(SUMS, cols)],
        [VMEM] * 3,
        [mine, other, sums],
    )
    return psi, norms[:ITERS, 0]


def solution(mesh):
    torus = Mesh(mesh.devices.reshape(NY, NX, NZ, NC), AXES)
    placed = (
        P(SECTOR, None, None),
        P(SECTOR_TERM, None, None),
        P(SECTOR_TERM, None, None),
        P(SECTOR_TERM),
        P(SECTOR_TERM),
        P(SECTOR, None, None),
        P(),
    )
    return jax.shard_map(
        per_device,
        mesh=torus,
        in_specs=placed,
        out_specs=(P(SECTOR, None, None), P()),
        check_vma=False,
    )
```
